32 devices in a mesh: row: 8 (over z, x), col: 4 (over y, core).
Axes of the slice: x: 2, y: 2, z: 4, core: 2. Of those that a mesh axis runs over, the one named last changes fastest.
Arguments:
- gradient: bfloat16 [3072, 14336], P('row', 'col'), may hold values from -0.1875 to 0.1875
- left_factor: float32 [3072, 3072], P('row', 'col'), may hold values from -1 to 11, as said below
- right_factor: float32 [14336, 14336], P('col', 'row'), may hold values from -1 to 3, as said below
- left_basis: bfloat16 [3072, 3072], P('row', 'col'), may hold values from -0.109375 to 0.109375
- right_basis: bfloat16 [14336, 2048], P('row', 'col'), may hold values from -0.046875 to 0.046875
Outputs:
- left_new: float32 [3072, 3072], P('row', 'col')
- right_new: float32 [14336, 14336], P('col', 'row')
- left_out: float32 [3072, 3072], P('row', 'col')
- right_out: float32 [14336, 2048], P('col', 'row')
The draws below stay inside these ranges and needn't reach their ends.
Inputs may be any that keep to these rules, and one draw needn't show every extreme that they name: left_factor is symmetric. right_factor is symmetric.
All inputs are finite; a program needn't handle non-finite values.
Results may differ from the reference program's by a relative error of at most 0.0029.
Values may be sent and summed in bfloat16 or wider, within the bound.
A program may use at most 192 MiB of HBM per device.

```python
import math
import jax
import jax.numpy as jnp
from jax import lax

DMODEL = 3072
DHIDDEN = 14336
NVEC = 2048


def factor_draw(key, size, level):
    noise = jax.random.truncated_normal(jax.random.fold_in(key, 11), -4.0, 4.0, (size, size), jnp.float32)
    noise = noise * (0.4 / math.sqrt(size))
    symmetric = noise + noise.T
    place = jnp.arange(size, dtype=jnp.float32) / size
    spread = jax.random.uniform(jax.random.fold_in(key, 12), (size,), jnp.float32, -1.2, 1.2)
    scaling = jnp.sqrt(level * jnp.exp(math.log(3.0) * place + spread))
    base = jnp.eye(size, dtype=jnp.float32) + symmetric
    return scaling[:, None] * base * scaling[None, :]


def draw_left_factor(key, part):
    return factor_draw(jax.random.fold_in(key, 21), DMODEL, 1.0)


def draw_right_factor(key, part):
    return factor_draw(jax.random.fold_in(key, 22), DHIDDEN, DMODEL / DHIDDEN)


def steps_of(own_key, shape, shards, least, top_value):
    loudness, own = 1.0, jax.random.fold_in(own_key, 6)
    for position, shards_of in shards:
        heights = jnp.exp(jax.random.uniform(jax.random.fold_in(own, position), (shards_of,), jnp.float32, least / len(shards), top_value / len(shards)))
        loudness = loudness * jnp.repeat(heights, shape[position] // shards_of).reshape([-1 if axis == position else 1 for axis in range(len(shape))])
    return loudness


def scatter_about(stream_key, extent, scale, limit, pieces=(), held_as=jnp.bfloat16):
    array = jax.random.normal(stream_key, extent, jnp.float32) * scale
    if len(pieces) > 0:
        array = steps_of(stream_key, extent, pieces, -0.22, 0.18) * array
    return jnp.clip(array, min=-limit, max=limit).astype(held_as)


def setup_inputs(seed: int = 0) -> dict:
    streams_of = jax.random.split(jax.random.key(seed), 6)
    return {
        "gradient": scatter_about(streams_of[0], (DMODEL, DHIDDEN), (DHIDDEN // 16) ** -0.5, 0.1875, ((0, 8), (1, 4))),
        "left_factor": draw_left_factor(jax.random.fold_in(streams_of[5], 71), 0),
        "right_factor": draw_right_factor(jax.random.fold_in(streams_of[5], 71), 0),
        "left_basis": scatter_about(streams_of[3], (DMODEL, DMODEL), DMODEL ** -0.5, 0.109375, ((0, 8), (1, 4))),
        "right_basis": scatter_about(streams_of[4], (DHIDDEN, NVEC), DHIDDEN ** -0.5, 0.046875, ((0, 8), (1, 4))),
    }


ema_decay = 0.95
epsilon = 1e-06

def reference(gradient, left_factor, right_factor, left_basis, right_basis):
    gram_left = lax.dot_general(gradient, gradient, (((1,), (1,)), ((), ())), preferred_element_type=jnp.float32)
    gram_right = lax.dot_general(gradient, gradient, (((0,), (0,)), ((), ())), preferred_element_type=jnp.float32)
    left_new = ema_decay * left_factor + (1.0 - ema_decay) * gram_left
    right_new = ema_decay * right_factor + (1.0 - ema_decay) * gram_right
    left_half = left_new.astype(jnp.bfloat16)
    right_half = right_new.astype(jnp.bfloat16)
    left_prod = jnp.dot(left_half, left_basis, preferred_element_type=jnp.float32)
    right_prod = jnp.dot(right_half, right_basis, preferred_element_type=jnp.float32)
    left_sq = lax.optimization_barrier(jnp.sum(left_prod * left_prod, axis=0))
    right_sq = lax.optimization_barrier(jnp.sum(right_prod * right_prod, axis=0))
    left_out = left_prod * lax.rsqrt(left_sq / DMODEL + epsilon)
    right_out = right_prod * lax.rsqrt(right_sq / DHIDDEN + epsilon)
    return (left_new, right_new, left_out, right_out)
```

```python
import functools

import jax
import jax.numpy as jnp
from jax import lax
from jax.experimental import pallas as pl
from jax.experimental.pallas import tpu as pltpu
from jax.sharding import PartitionSpec as P

ema_decay = 0.95
epsilon = 1e-06
MESH = pl.DeviceIdType.MESH
SLOTS = 4


def dot(a, b, dims):
    return lax.dot_general(a, b, (dims, ((), ())), preferred_element_type=jnp.float32)


def place_of(row, row_count):
    half = lax.div(row, 2)
    return jnp.where(lax.rem(row, 2) == 0, half, row_count - 1 - half)


def member_at(place, row_count):
    return jnp.where(place < row_count // 2, 2 * place, 2 * (row_count - 1 - place) + 1)


def greet(peers):
    barrier = pltpu.get_barrier_semaphore()
    for peer in peers:
        pl.semaphore_signal(barrier, inc=1, device_id=peer, device_id_type=MESH)
    pl.semaphore_wait(barrier, len(peers))


def gather_kernel(
    R, C, tile,
    grad, lb, rb, rf,
    right_out, left_out, lb_out, rb_out, match,
    acc, slab, own, rhs, left,
    load_sem, rf_sem, ring_send, ring_recv, match_send, match_recv, rhs_sem,
    lb_send, lb_recv, rb_send, rb_recv, keep_sem, out_sem,
):
    row, col = lax.axis_index("row"), lax.axis_index("col")
    rows, cols = grad.shape
    half = rows // 2
    ratio = R // C
    part = cols // ratio
    here = place_of(row, R)
    nxt = member_at(lax.rem(here + 1, R), R)
    prv = member_at(lax.rem(here + R - 1, R), R)
    toward = (nxt, prv)
    owner = lax.div(row, ratio)
    chosen = lax.rem(row, ratio)
    offset = lax.rem(col + C - owner, C)
    is_owner = offset == 0
    is_relay = jnp.logical_and(offset != 0, lax.rem(offset, 2) == 0)
    partner = col + 1 - 2 * lax.rem(col, 2)

    def origin(direction, t):
        there = here + R - t if direction == 0 else here + t
        return member_at(lax.rem(there, R), R)

    loads = []
    for s in range(ratio):
        lanes = pl.ds(s * part, part)
        for d in range(2):
            loads.append(pltpu.make_async_copy(
                grad.at[pl.ds(d * half, half), lanes], slab.at[0, d, s], load_sem.at[d, s]))
        loads.append(pltpu.make_async_copy(grad.at[:, lanes], own.at[s], load_sem.at[2, s]))
    for load in loads:
        load.start()
    load_rf = pltpu.make_async_copy(rf, acc, rf_sem)
    load_rf.start()
    keep_lb = pltpu.make_async_copy(
        lb, lb_out.at[pl.ds(pl.multiple_of(row * rows, 32), rows)], keep_sem.at[0])
    keep_rb = pltpu.make_async_copy(rb, rb_out.at[col], keep_sem.at[1])

    greet([{"row": nxt}, {"row": prv}] + [{"col": lax.rem(col + j, C)} for j in range(1, C)])

    def ring(t, d, s):
        return pltpu.make_async_remote_copy(
            src_ref=slab.at[t % SLOTS, d, s],
            dst_ref=slab.at[(t + 1) % SLOTS, d, s],
            send_sem=ring_send.at[t % 2, d, s],
            recv_sem=ring_recv.at[(t + 1) % SLOTS, d, s],
            device_id={"row": toward[d]}, device_id_type=MESH)

    def match_copy(t, d, j, source):
        target = partner if j == 0 else lax.rem(col + 2 * j, C)
        return pltpu.make_async_remote_copy(
            src_ref=source, dst_ref=match.at[t, d],
            send_sem=match_send.at[t % 2, d, j], recv_sem=match_recv.at[t, d],
            device_id={"col": target}, device_id_type=MESH)

    def offers(t):
        return [match_copy(t, d, j, slab.at[t % SLOTS, d, chosen])
                for d in range(2) for j in list(range(1, C // 2)) + [0]]

    def relays(t):
        return [match_copy(t, d, 0, match.at[t, d]) for d in range(2)]

    def offer(t):
        @pl.when(is_owner)
        def _():
            for copy in offers(t):
                copy.start()

    def settle(t):
        @pl.when(is_owner)
        def _():
            for copy in offers(t):
                copy.wait_send()

        @pl.when(is_relay)
        def _():
            for copy in relays(t):
                copy.wait_send()

    def relay(t):
        @pl.when(is_relay)
        def _():
            for copy in relays(t):
                copy.wait_recv()
                copy.start()

    def bring(t):
        @pl.when(is_owner)
        def _():
            for d in range(2):
                rhs[t % 2, d] = slab[t % SLOTS, d, chosen]

        @pl.when(jnp.logical_not(is_owner))
        def _():
            @pl.when(jnp.logical_not(is_relay))
            def _():
                for copy in relays(t):
                    copy.wait_recv()

            copies = [pltpu.make_async_copy(match.at[t, d], rhs.at[t % 2, d], rhs_sem.at[d])
                      for d in range(2)]
            for copy in copies:
                copy.start()
            for copy in copies:
                copy.wait()

    def write(row0):
        return pltpu.make_async_copy(
            acc.at[pl.ds(row0, tile)], right_out.at[pl.ds(row0, tile)], out_sem)

    def gram(t, s):
        @pl.loop(0, part // tile)
        def _(j):
            first = pl.multiple_of(j * tile, tile)
            block = jnp.concatenate(
                [slab[t % SLOTS, d, s, :, pl.ds(first, tile)] for d in range(2)], axis=0).T
            row0 = pl.multiple_of(s * part + j * tile, tile)
            for n in range(part // tile):
                lanes = slice(n * tile, (n + 1) * tile)
                other = rhs[t % 2, :, :, lanes].reshape(rows, tile)
                acc[pl.ds(row0, tile), lanes] += (1.0 - ema_decay) * dot(block, other, ((1,), (0,)))
            if t == R - 1:
                write(row0).start()

    def gram_left(t):
        for d in range(2):
            total = None
            for s in range(ratio):
                term = dot(slab[t % SLOTS, d, s], own[s], ((1,), (1,)))
                total = term if total is None else total + term
            row0 = pl.multiple_of(origin(d, t) * rows + d * half, 32)
            left[pl.ds(row0, half), :] = total

    def basis_ring(j, d):
        at = pl.ds(pl.multiple_of(origin(d, j) * rows + d * half, 32), half)
        return pltpu.make_async_remote_copy(
            src_ref=lb.at[pl.ds(d * half, half)] if j == 0 else lb_out.at[at],
            dst_ref=lb_out.at[at],
            send_sem=lb_send.at[j % 2, d], recv_sem=lb_recv.at[j, d],
            device_id={"row": toward[d]}, device_id_type=MESH)

    def basis_hop(j):
        for d in range(2):
            if j > 0:
                basis_ring(j - 1, d).wait_recv()
            if j < R - 1:
                if j > 1:
                    basis_ring(j - 2, d).wait_send()
                basis_ring(j, d).start()

    def vectors(j):
        target = partner if j == 0 else lax.rem(col + 2 * j, C)
        return pltpu.make_async_remote_copy(
            src_ref=rb, dst_ref=rb_out.at[col], send_sem=rb_send.at[0, j], recv_sem=rb_recv.at[col],
            device_id={"col": target}, device_id_type=MESH)

    def vectors_on(j):
        source = lax.rem(col + 2 * j, C)
        return pltpu.make_async_remote_copy(
            src_ref=rb_out.at[source], dst_ref=rb_out.at[source],
            send_sem=rb_send.at[1, j], recv_sem=rb_recv.at[source],
            device_id={"col": partner}, device_id_type=MESH)

    def vectors_in(source):
        return pltpu.make_async_remote_copy(
            src_ref=rb, dst_ref=rb_out.at[source], send_sem=rb_send.at[0, 0], recv_sem=rb_recv.at[source],
            device_id={"col": partner}, device_id_type=MESH)

    for load in loads:
        load.wait()
    for s in range(ratio):
        for d in range(2):
            ring(0, d, s).start()
    offer(0)
    keep_lb.start()
    keep_rb.start()
    for j in range(C // 2):
        vectors(j).start()
    load_rf.wait()

    @pl.loop(0, cols // tile)
    def _(j):
        at = pl.ds(pl.multiple_of(j * tile, tile), tile)
        acc[at, :] = acc[at, :] * ema_decay

    begin = R // 2
    for t in range(1, R):
        for s in range(ratio):
            for d in range(2):
                ring(t - 1, d, s).wait_recv()
            if t < R - 1:
                for d in range(2):
                    ring(t, d, s).start()

            if s == ratio - 1:
                offer(t)
                if t >= begin:
                    basis_hop(t - begin)
            if s == 0:
                relay(t - 1)
                bring(t - 1)
            gram(t - 1, s)
            if s == ratio - 1:
                gram_left(t - 1)
                settle(t - 1)
            for d in range(2):
                ring(t - 1, d, s).wait_send()
        if t == R // 2 - 1:
            for j in range(1, C // 2):
                vectors_in(lax.rem(col + 2 * j, C)).wait_recv()
                vectors_on(j).start()
    last = R - 1
    hops = list(range(R - begin, R))
    basis_hop(hops.pop(0))
    relay(last)
    if hops:
        basis_hop(hops.pop(0))
    bring(last)
    gram_left(last)
    put_left = pltpu.make_async_copy(left, left_out, keep_sem.at[2])
    put_left.start()
    for s in range(ratio):
        gram(last, s)
        if hops:
            basis_hop(hops.pop(0))
    settle(last)
    for hop in hops:
        basis_hop(hop)
    for d in range(2):
        for j in range(max(R - 3, 0), R - 1):
            basis_ring(j, d).wait_send()
    keep_lb.wait()
    keep_rb.wait()
    vectors_in(partner).wait_recv()
    for j in range(1, C // 2):
        vectors_in(lax.rem(partner + 2 * j, C)).wait_recv()
        vectors_on(j).wait_send()
    for j in range(C // 2):
        vectors(j).wait_send()
    put_left.wait()
    pltpu.make_async_copy(acc, right_out, out_sem).wait()


def gather_stage(R, C, gradient, left_basis, right_basis, right_factor):
    rows, cols = gradient.shape
    half, ratio = rows // 2, R // C
    part = cols // ratio
    tile = 256 if part % 256 == 0 else 128
    dmodel = rows * R
    any_space = pl.BlockSpec(memory_space=pl.ANY)
    dma = pltpu.SemaphoreType.DMA
    return pl.pallas_call(
        functools.partial(gather_kernel, R, C, tile),
        out_shape=(
            jax.ShapeDtypeStruct(right_factor.shape, jnp.float32),
            jax.ShapeDtypeStruct((dmodel, rows), jnp.float32),
            jax.ShapeDtypeStruct((dmodel, left_basis.shape[1]), jnp.bfloat16),
            jax.ShapeDtypeStruct((C,) + right_basis.shape, jnp.bfloat16),
            jax.ShapeDtypeStruct((R, 2, half, part), jnp.bfloat16),
        ),
        in_specs=[any_space] * 4,
        out_specs=(any_space,) * 5,
        scratch_shapes=[
            pltpu.VMEM(right_factor.shape, jnp.float32),
            pltpu.VMEM((SLOTS, 2, ratio, half, part), jnp.bfloat16),
            pltpu.VMEM((ratio, rows, part), jnp.bfloat16),
            pltpu.VMEM((2, 2, half, part), jnp.bfloat16),
            pltpu.VMEM((dmodel, rows), jnp.float32),
            dma((3, ratio)), dma, dma((2, 2, ratio)), dma((SLOTS, 2, ratio)),
            dma((2, 2, C // 2)), dma((R, 2)), dma((2,)),
            dma((2, 2)), dma((R - 1, 2)), dma((2, C // 2)), dma((C,)), dma((3,)), dma,
        ],
        compiler_params=pltpu.CompilerParams(
            collective_id=0, has_side_effects=True, vmem_limit_bytes=62 * 1024 * 1024),
        name="gather_gram",
    )(gradient, left_basis, right_basis, right_factor)


def product_kernel(
    R, C, m, dhidden,
    fresh, vectors, left_part, basis, left_factor,
    right_out, left_new_out, left_out,
    bv, xf, xh, rbuf, sbuf, prod, square, gather_sq,
    lparts, lhalf, lbasis, lfac, lnew, lprod, lsq,
    load_sem, x_sem, send_sem, recv_sem, sq_send, sq_recv,
    lp_send, lp_recv, lh_send, lh_recv, ls_send, ls_recv, out_sem,
):
    row, col = lax.axis_index("row"), lax.axis_index("col")
    total_rows, depth = fresh.shape
    lcols = left_factor.shape[1]
    dmodel = basis.shape[0]
    width = prod.shape[1]
    ratio = R // C
    H = R // 2
    count = total_rows // m
    hm = m // 2
    keep = xh.shape[0]
    here = place_of(row, R)
    toward = tuple(member_at(lax.rem(here + step, R), R) for step in (1, R - 1))

    load_v = pltpu.make_async_copy(vectors, bv, load_sem.at[0])
    load_b = pltpu.make_async_copy(basis, lbasis, load_sem.at[1])
    load_f = pltpu.make_async_copy(left_factor, lfac, load_sem.at[2])
    mine = pl.ds(pl.multiple_of(col * lcols, 128), lcols)
    load_p = pltpu.make_async_copy(left_part.at[mine], lparts.at[col], load_sem.at[3])
    load_v.start()

    def chunk(k):
        return pltpu.make_async_copy(
            fresh.at[pl.ds(pl.multiple_of(k * m, m), m)], xf.at[lax.rem(k, 2)], x_sem.at[lax.rem(k, 2)])

    chunk(0).start()
    load_b.start()
    load_f.start()
    load_p.start()
    greet([{"row": lax.rem(row + j, R)} for j in range(1, R)]
          + [{"col": lax.rem(col + j, C)} for j in range(1, C)])

    def other_col(j):
        return lax.rem(col + j, C)

    def part_copy(j):
        there = other_col(j)
        at = pl.ds(pl.multiple_of(there * lcols, 128), lcols)
        return pltpu.make_async_remote_copy(
            src_ref=left_part.at[at], dst_ref=lparts.at[col],
            send_sem=lp_send.at[j], recv_sem=lp_recv.at[col],
            device_id={"col": there}, device_id_type=MESH)

    def part_in(j):
        source = other_col(j)
        return pltpu.make_async_remote_copy(
            src_ref=left_part.at[mine], dst_ref=lparts.at[source],
            send_sem=lp_send.at[j], recv_sem=lp_recv.at[source],
            device_id={"col": source}, device_id_type=MESH)

    def half_copy(j, source):
        return pltpu.make_async_remote_copy(
            src_ref=lhalf.at[source], dst_ref=lhalf.at[source],
            send_sem=lh_send.at[j], recv_sem=lh_recv.at[source],
            device_id={"col": other_col(j)}, device_id_type=MESH)

    def lsq_copy(j, source):
        return pltpu.make_async_remote_copy(
            src_ref=lsq.at[source], dst_ref=lsq.at[source],
            send_sem=ls_send.at[j], recv_sem=ls_recv.at[source],
            device_id={"row": lax.rem(row + j, R)}, device_id_type=MESH)

    def sq_copy(j, source):
        return pltpu.make_async_remote_copy(
            src_ref=gather_sq.at[source], dst_ref=gather_sq.at[source],
            send_sem=sq_send.at[j], recv_sem=sq_recv.at[source],
            device_id={"col": other_col(j)}, device_id_type=MESH)

    new_out = pltpu.make_async_copy(lnew, left_new_out, out_sem.at[0])
    prod_out = pltpu.make_async_copy(lprod, left_out, out_sem.at[1])

    def left_sum():
        load_p.wait()
        load_f.wait()
        for j in range(1, C):
            part_in(j).wait_recv()
        total = lparts[0]
        for c in range(1, C):
            total = total + lparts[c]
        value = ema_decay * lfac[...] + (1.0 - ema_decay) * total.T
        lnew[...] = value
        lhalf[col] = value.astype(jnp.bfloat16)
        new_out.start()
        for j in range(1, C):
            half_copy(j, col).start()

    def left_product():
        load_b.wait()
        for j in range(1, C):
            half_copy(j, other_col(j)).wait_recv()
        total = None
        for c in range(C):
            term = dot(lhalf[c], lbasis[c * lcols:(c + 1) * lcols], ((1,), (0,)))
            total = term if total is None else total + term
        lprod[...] = total
        lsq[row] = jnp.broadcast_to(jnp.sum(total * total, axis=0, keepdims=True), lsq.shape[1:])
        for j in range(1, R):
            lsq_copy(j, row).start()

    def left_finish():
        for j in range(1, R):
            lsq_copy(j, lax.rem(row + j, R)).wait_recv()
        total = lsq[0]
        for r in range(1, R):
            total = total + lsq[r]
        lprod[...] = lprod[...] * lax.rsqrt(total[0:1] / dmodel + epsilon)
        prod_out.start()

    def message(t, d, h):
        rows = pl.ds(d * hm, hm) if h == 0 else pl.ds(0, m)
        return pltpu.make_async_remote_copy(
            src_ref=sbuf.at[lax.rem(t, 2), d, h, rows],
            dst_ref=rbuf.at[lax.rem(t, 4), d, h, rows],
            send_sem=send_sem.at[lax.rem(t, 2), d, h],
            recv_sem=recv_sem.at[lax.rem(t, 4), d, h],
            device_id={"row": toward[d]}, device_id_type=MESH)

    def block(k, dest, rows):
        source = lax.div(dest, ratio)
        lanes = pl.ds(pl.multiple_of(lax.rem(dest, ratio) * width, 128), width)
        return dot(xh[lax.rem(k, keep), rows], bv[source, :, lanes], ((1,), (0,)))

    def dest_of(d, h):
        away = H - h if d == 0 else R - (H - h)
        return member_at(lax.rem(here + away, R), R)

    def ready(k):
        return jnp.logical_and(k >= 0, k < count)

    for j in range(1, C):
        part_copy(j).start()
    square[...] = jnp.zeros_like(square)
    load_v.wait()
    steps = count + H

    @pl.loop(0, steps)
    def _(t):
        @pl.when(t < count)
        def _():
            chunk(t).wait()

            @pl.when(t + 1 < count)
            def _():
                chunk(t + 1).start()

            xh[lax.rem(t, keep)] = xf[lax.rem(t, 2)].astype(jnp.bfloat16)

        @pl.when(ready(t - H))
        def _():
            k = t - H
            total = block(k, row, slice(0, m))
            for d in range(2):
                message(t - 1, d, H - 1).wait_recv()
                total = total + rbuf[lax.rem(t - 1, 4), d, H - 1].astype(jnp.float32)
            prod[pl.ds(pl.multiple_of(k * m, m), m), :] = total
            square[...] += jnp.sum(total * total, axis=0, keepdims=True)

        for h in range(H - 1, -1, -1):
            @pl.when(ready(t - h))
            def _():
                k = t - h
                for d in range(2):
                    @pl.when(k >= 2)
                    def _():
                        message(t - 2, d, h).wait_send()

                    dest = dest_of(d, h)
                    slot = lax.rem(t, 2)
                    some = slice(d * hm, d * hm + hm)
                    rest = slice(hm - d * hm, m - d * hm)
                    if h == 0:
                        sbuf[slot, d, h, some] = block(k, dest, some).astype(jnp.bfloat16)
                    else:
                        fresh_part = block(k, dest, slice(0, m))
                        message(t - 1, d, h - 1).wait_recv()
                        if h == 1:
                            came = rbuf[lax.rem(t - 1, 4), d, 0, some].astype(jnp.float32)
                            sbuf[slot, d, h, some] = (fresh_part[some] + came).astype(jnp.bfloat16)
                            sbuf[slot, d, h, rest] = fresh_part[rest].astype(jnp.bfloat16)
                        else:
                            came = rbuf[lax.rem(t - 1, 4), d, h - 1].astype(jnp.float32)
                            sbuf[slot, d, h] = (fresh_part + came).astype(jnp.bfloat16)
                    message(t, d, h).start()

        for at, work in ((6, left_sum), (8, left_product), (10, left_finish)):
            pl.when(t == min(at, steps - 1))(work)

    gather_sq[col] = jnp.broadcast_to(square[...], gather_sq.shape[1:])
    for j in range(1, C):
        sq_copy(j, col).start()
    for d in range(2):
        for h in range(H):
            for k in (count - 2, count - 1):
                message(k + h, d, h).wait_send()
    for j in range(1, C):
        part_copy(j).wait_send()
        half_copy(j, col).wait_send()
    for j in range(1, R):
        lsq_copy(j, row).wait_send()
    new_out.wait()
    prod_out.wait()
    for j in range(1, C):
        sq_copy(j, other_col(j)).wait_recv()
    total = gather_sq[0]
    for c in range(1, C):
        total = total + gather_sq[c]
    scale = lax.rsqrt(total[0:1] / dhidden + epsilon)

    def put(k):
        at = pl.ds(pl.multiple_of(k * m, m), m)
        return pltpu.make_async_copy(prod.at[at], right_out.at[at], out_sem.at[2])

    @pl.loop(0, count)
    def _(k):
        at = pl.ds(pl.multiple_of(k * m, m), m)
        prod[at, :] = prod[at, :] * scale
        put(k).start()

    for j in range(1, C):
        sq_copy(j, col).wait_send()
    pltpu.make_async_copy(prod, right_out, out_sem.at[2]).wait()


def product_stage(R, C, dhidden, fresh, vectors, left_part, basis, left_factor):
    total_rows, depth = fresh.shape
    m = 256
    H = R // 2
    width = vectors.shape[0] * vectors.shape[2] // R
    rows, lcols = left_factor.shape
    any_space = pl.BlockSpec(memory_space=pl.ANY)
    dma = pltpu.SemaphoreType.DMA
    f32, bf16 = jnp.float32, jnp.bfloat16
    return pl.pallas_call(
        functools.partial(product_kernel, R, C, m, dhidden),
        out_shape=(
            jax.ShapeDtypeStruct((total_rows, width), f32),
            jax.ShapeDtypeStruct((rows, lcols), f32),
            jax.ShapeDtypeStruct((rows, lcols), f32),
        ),
        in_specs=[any_space] * 5,
        out_specs=(any_space,) * 3,
        scratch_shapes=[
            pltpu.VMEM(vectors.shape, bf16),
            pltpu.VMEM((2, m, depth), f32),
            pltpu.VMEM((H + 1, m, depth), bf16),
            pltpu.VMEM((4, 2, H, m, width), bf16),
            pltpu.VMEM((2, 2, H, m, width), bf16),
            pltpu.VMEM((total_rows, width), f32),
            pltpu.VMEM((1, width), f32),
            pltpu.VMEM((C, 8, width), f32),
            pltpu.VMEM((C, lcols, rows), f32),
            pltpu.VMEM((C, rows, lcols), bf16),
            pltpu.VMEM(basis.shape, bf16),
            pltpu.VMEM((rows, lcols), f32),
            pltpu.VMEM((rows, lcols), f32),
            pltpu.VMEM((rows, lcols), f32),
            pltpu.VMEM((R, 8, lcols), f32),
            dma((4,)), dma((2,)), dma((2, 2, H)), dma((4, 2, H)), dma((C,)), dma((C,)),
            dma((C,)), dma((C,)), dma((C,)), dma((C,)), dma((R,)), dma((R,)), dma((3,)),
        ],
        compiler_params=pltpu.CompilerParams(
            collective_id=1, has_side_effects=True, vmem_limit_bytes=62 * 1024 * 1024),
        name="product_reduce",
    )(fresh, vectors, left_part, basis, left_factor)


def make_body(R, C, dhidden):
    def on_device(gradient, left_factor, right_factor, left_basis, right_basis):
        right_new, gram_part, left_basis_cols, vectors, _ = gather_stage(
            R, C, gradient, left_basis, right_basis, right_factor)
        right_out, left_new, left_out = product_stage(
            R, C, dhidden, right_new, vectors, gram_part, left_basis_cols, left_factor)
        return (left_new, right_new, left_out, right_out)

    return on_device


def solution(mesh):
    in_specs = (P("row", "col"), P("row", "col"), P("col", "row"), P("row", "col"), P("row", "col"))
    out_specs = (P("row", "col"), P("col", "row"), P("row", "col"), P("col", "row"))

    def step(gradient, left_factor, right_factor, left_basis, right_basis):
        body = make_body(mesh.shape["row"], mesh.shape["col"], gradient.shape[1])
        return jax.shard_map(
            body, mesh=mesh, in_specs=in_specs, out_specs=out_specs, check_vma=False
        )(gradient, left_factor, right_factor, left_basis, right_basis)

    return step
```

```python
import functools

import jax
import jax.numpy as jnp
from jax import lax
from jax.experimental import pallas as pl
from jax.experimental.pallas import tpu as pltpu
from jax.sharding import PartitionSpec as P

ema_decay = 0.95
epsilon = 1e-06
MESH = pl.DeviceIdType.MESH
SLOTS = 4
SPLIT = 2
CHUNK = 256


def dot(a, b, dims):
    return lax.dot_general(a, b, (dims, ((), ())), preferred_element_type=jnp.float32)


def place_of(row, row_count):
    half = lax.div(row, 2)
    return jnp.where(lax.rem(row, 2) == 0, half, row_count - 1 - half)


def member_at(place, row_count):
    return jnp.where(place < row_count // 2, 2 * place, 2 * (row_count - 1 - place) + 1)


def greet(peers):
    barrier = pltpu.get_barrier_semaphore()
    for peer in peers:
        pl.semaphore_signal(barrier, inc=1, device_id=peer, device_id_type=MESH)
    pl.semaphore_wait(barrier, len(peers))


def gather_kernel(
    R, C, tile,
    grad, lb, rb, rf,
    partial_out, left_out, lb_out, rb_out, last_out, last_match, match,
    acc, slab, own, rhs, left,
    load_sem, rf_sem, ring_send, ring_recv, match_send, match_recv, rhs_sem,
    lb_send, lb_recv, rb_send, rb_recv, keep_sem, out_sem,
):
    row, col = lax.axis_index("row"), lax.axis_index("col")
    rows, cols = grad.shape
    half = rows // 2
    ratio = R // C
    part = cols // ratio
    here = place_of(row, R)
    nxt = member_at(lax.rem(here + 1, R), R)
    prv = member_at(lax.rem(here + R - 1, R), R)
    toward = (nxt, prv)
    owner = lax.div(row, ratio)
    quarter = half // SPLIT
    chosen = pl.ds(pl.multiple_of(lax.rem(row, ratio) * part, 128), part)
    last = R - 1
    offset = lax.rem(col + C - owner, C)
    is_owner = offset == 0
    is_relay = jnp.logical_and(offset != 0, lax.rem(offset, 2) == 0)
    partner = col + 1 - 2 * lax.rem(col, 2)

    def origin(direction, t):
        there = here + R - t if direction == 0 else here + t
        return member_at(lax.rem(there, R), R)

    loads = [pltpu.make_async_copy(grad, own, load_sem.at[2, 0])]
    for s in range(SPLIT):
        for d in range(2):
            loads.append(pltpu.make_async_copy(
                grad.at[pl.ds(d * half + s * quarter, quarter)], slab.at[0, d, s], load_sem.at[d, s]))
    for load in reversed(loads):
        load.start()
    load_rf = pltpu.make_async_copy(rf, acc, rf_sem)
    load_rf.start()
    keep_lb = pltpu.make_async_copy(
        lb, lb_out.at[pl.ds(pl.multiple_of(row * rows, 32), rows)], keep_sem.at[0])
    keep_rb = pltpu.make_async_copy(rb, rb_out.at[col], keep_sem.at[1])

    greet([{"row": nxt}, {"row": prv}] + [{"col": lax.rem(col + j, C)} for j in range(1, C)])

    def ring(t, d, s):
        return pltpu.make_async_remote_copy(
            src_ref=slab.at[t % SLOTS, d, s],
            dst_ref=slab.at[(t + 1) % SLOTS, d, s],
            send_sem=ring_send.at[t % 2, d, s],
            recv_sem=ring_recv.at[(t + 1) % SLOTS, d, s],
            device_id={"row": toward[d]}, device_id_type=MESH)

    def landed(t, d, s):
        return last_match.at[d, s] if t == last else match.at[t, d, s]

    def match_copy(t, d, s, j, source):
        target = partner if j == 0 else lax.rem(col + 2 * j, C)
        return pltpu.make_async_remote_copy(
            src_ref=source, dst_ref=landed(t, d, s),
            send_sem=match_send.at[t % 2, d, s, j], recv_sem=match_recv.at[t, d, s],
            device_id={"col": target}, device_id_type=MESH)

    def offers(t, s):
        return [match_copy(t, d, s, j, slab.at[t % SLOTS, d, s, :, chosen])
                for d in range(2) for j in list(range(1, C // 2)) + [0]]

    def relays(t, s):
        return [match_copy(t, d, s, 0, landed(t, d, s)) for d in range(2)]

    def offer(t, s):
        @pl.when(is_owner)
        def _():
            for copy in offers(t, s):
                copy.start()

    def settle(t):
        for s in range(SPLIT):
            @pl.when(is_owner)
            def _():
                for copy in offers(t, s):
                    copy.wait_send()

            @pl.when(is_relay)
            def _():
                for copy in relays(t, s):
                    copy.wait_send()

    def relay(t, s):
        @pl.when(is_relay)
        def _():
            for copy in relays(t, s):
                copy.wait_recv()
                copy.start()

    def arrive(t):
        @pl.when(jnp.logical_not(jnp.logical_or(is_owner, is_relay)))
        def _():
            for s in range(SPLIT):
                for copy in relays(t, s):
                    copy.wait_recv()

    def bring(t):
        arrive(t)

        @pl.when(is_owner)
        def _():
            for d in range(2):
                for s in range(SPLIT):
                    rhs[t % 2, d, s] = slab[t % SLOTS, d, s, :, chosen]

        @pl.when(jnp.logical_not(is_owner))
        def _():
            copy = pltpu.make_async_copy(match.at[t], rhs.at[t % 2], rhs_sem.at[0])
            copy.start()
            copy.wait()

    def write(row0):
        return pltpu.make_async_copy(
            acc.at[pl.ds(row0, tile)], partial_out.at[pl.ds(row0, tile)], out_sem)

    def gram(t, s):
        @pl.loop(0, part // tile)
        def _(j):
            first = pl.multiple_of(j * tile, tile)
            row0 = pl.multiple_of(s * part + first, tile)
            block = slab[t % SLOTS, :, :, :, pl.ds(row0, tile)].reshape(rows, tile).T
            for n in range(part // tile):
                lanes = slice(n * tile, (n + 1) * tile)
                other = rhs[t % 2, :, :, :, lanes].reshape(rows, tile)
                acc[pl.ds(row0, tile), lanes] += (1.0 - ema_decay) * dot(block, other, ((1,), (0,)))
            if t == last - 1:
                write(row0).start()

    def gram_left(t):
        for d in range(2):
            total = dot(slab[t % SLOTS, d].reshape(half, cols), own[...], ((1,), (1,)))
            row0 = pl.multiple_of(origin(d, t) * rows + d * half, 32)
            left[pl.ds(row0, half), :] = total

    def basis_ring(j, d):
        at = pl.ds(pl.multiple_of(origin(d, j) * rows, 32), rows)
        return pltpu.make_async_remote_copy(
            src_ref=lb if j == 0 else lb_out.at[at], dst_ref=lb_out.at[at],
            send_sem=lb_send.at[j % 2, d], recv_sem=lb_recv.at[j, d],
            device_id={"row": toward[d]}, device_id_type=MESH)

    def basis_hop(j):
        for d in range(2):
            if j > 0:
                basis_ring(j - 1, d).wait_recv()
        for d in range(2):
            if j < hops:
                if j > 1:
                    basis_ring(j - 2, d).wait_send()
                basis_ring(j, d).start()

    def vectors(j):
        target = partner if j == 0 else lax.rem(col + 2 * j, C)
        return pltpu.make_async_remote_copy(
            src_ref=rb, dst_ref=rb_out.at[col], send_sem=rb_send.at[0, j], recv_sem=rb_recv.at[col],
            device_id={"col": target}, device_id_type=MESH)

    def vectors_on(j):
        source = lax.rem(col + 2 * j, C)
        return pltpu.make_async_remote_copy(
            src_ref=rb_out.at[source], dst_ref=rb_out.at[source],
            send_sem=rb_send.at[1, j], recv_sem=rb_recv.at[source],
            device_id={"col": partner}, device_id_type=MESH)

    def vectors_in(source):
        return pltpu.make_async_remote_copy(
            src_ref=rb, dst_ref=rb_out.at[source], send_sem=rb_send.at[0, 0], recv_sem=rb_recv.at[source],
            device_id={"col": partner}, device_id_type=MESH)

    for load in reversed(loads):
        load.wait()
    for s in range(SPLIT):
        for d in range(2):
            ring(0, d, s).start()
    for s in range(SPLIT):
        offer(0, s)
    keep_lb.start()
    keep_rb.start()
    for j in range(C // 2):
        vectors(j).start()
    load_rf.wait()

    @pl.loop(0, cols // tile)
    def _(j):
        at = pl.ds(pl.multiple_of(j * tile, tile), tile)
        acc[at, :] = acc[at, :] * ema_decay

    relay_due = [(0, s) for s in range(SPLIT)]
    hops = R // 2 - 2
    begin = R - hops
    for t in range(1, R):
        for s in range(SPLIT):
            for d in range(2):
                ring(t - 1, d, s).wait_recv()
            if t < last:
                for d in range(2):
                    ring(t, d, s).start()
            offer(t, s)
            if s == SPLIT - 1 and t >= begin:
                basis_hop(t - begin)
            for due in relay_due:
                relay(*due)
            relay_due = [(t, s)]
            if s == 0:
                bring(t - 1)
            if s < SPLIT - 1:
                gram(t - 1, s)
            else:
                for rest in range(s, ratio):
                    gram(t - 1, rest)
                gram_left(t - 1)
                settle(t - 1)
            for d in range(2):
                ring(t - 1, d, s).wait_send()
        if t == R // 2 - 1:
            for j in range(1, C // 2):
                vectors_in(lax.rem(col + 2 * j, C)).wait_recv()
                vectors_on(j).start()
    put_last = pltpu.make_async_copy(slab.at[last % SLOTS], last_out, keep_sem.at[3])
    put_last.start()
    own_match = pltpu.make_async_copy(slab.at[last % SLOTS, :, :, :, chosen], last_match, rhs_sem.at[1])

    @pl.when(is_owner)
    def _():
        own_match.start()

    gram_left(last)
    put_left = pltpu.make_async_copy(left, left_out, keep_sem.at[2])
    put_left.start()
    for due in relay_due:
        relay(*due)
    arrive(last)
    settle(last)
    basis_hop(hops)
    for d in range(2):
        for j in range(max(hops - 2, 0), hops):
            basis_ring(j, d).wait_send()

    @pl.when(is_owner)
    def _():
        own_match.wait()

    put_last.wait()
    keep_lb.wait()
    keep_rb.wait()
    vectors_in(partner).wait_recv()
    for j in range(1, C // 2):
        vectors_in(lax.rem(partner + 2 * j, C)).wait_recv()
        vectors_on(j).wait_send()
    for j in range(C // 2):
        vectors(j).wait_send()
    put_left.wait()
    pltpu.make_async_copy(acc, partial_out, out_sem).wait()


def gather_stage(R, C, gradient, left_basis, right_basis, right_factor):
    rows, cols = gradient.shape
    half, ratio = rows // 2, R // C
    part, quarter = cols // ratio, half // SPLIT
    tile = 256 if part % 256 == 0 else 128
    dmodel = rows * R
    any_space = pl.BlockSpec(memory_space=pl.ANY)
    dma = pltpu.SemaphoreType.DMA
    return pl.pallas_call(
        functools.partial(gather_kernel, R, C, tile),
        out_shape=(
            jax.ShapeDtypeStruct(right_factor.shape, jnp.float32),
            jax.ShapeDtypeStruct((dmodel, rows), jnp.float32),
            jax.ShapeDtypeStruct((dmodel, left_basis.shape[1]), jnp.bfloat16),
            jax.ShapeDtypeStruct((C,) + right_basis.shape, jnp.bfloat16),
            jax.ShapeDtypeStruct((2, SPLIT, quarter, cols), jnp.bfloat16),
            jax.ShapeDtypeStruct((2, SPLIT, quarter, part), jnp.bfloat16),
            jax.ShapeDtypeStruct((R - 1, 2, SPLIT, quarter, part), jnp.bfloat16),
        ),
        in_specs=[any_space] * 4,
        out_specs=(any_space,) * 7,
        scratch_shapes=[
            pltpu.VMEM(right_factor.shape, jnp.float32),
            pltpu.VMEM((SLOTS, 2, SPLIT, quarter, cols), jnp.bfloat16),
            pltpu.VMEM((rows, cols), jnp.bfloat16),
            pltpu.VMEM((2, 2, SPLIT, quarter, part), jnp.bfloat16),
            pltpu.VMEM((dmodel, rows), jnp.float32),
            dma((3, SPLIT)), dma, dma((2, 2, SPLIT)), dma((SLOTS, 2, SPLIT)),
            dma((2, 2, SPLIT, C // 2)), dma((R, 2, SPLIT)), dma((2,)),
            dma((2, 2)), dma((R - 1, 2)), dma((2, C // 2)), dma((C,)), dma((4,)), dma,
        ],
        compiler_params=pltpu.CompilerParams(
            collective_id=0, has_side_effects=True, vmem_limit_bytes=62 * 1024 * 1024),
        name="gather_gram",
    )(gradient, left_basis, right_basis, right_factor)


def product_kernel(
    R, C, m, dhidden,
    fresh, vectors, left_part, basis, came_forward, came_back, left_factor,
    right_out, square_out, left_new_out, left_out,
    bv, xf, xh, rbuf, sbuf, prod, square, gather_sq, sum_sq,
    lparts, lhalf, lbasis, lfac, lnew, lprod, lsq,
    load_sem, x_sem, send_sem, recv_sem, sq_send, sq_recv,
    lp_send, lp_recv, lh_send, lh_recv, ls_send, ls_recv, lb_send, lb_recv, out_sem,
):
    row, col = lax.axis_index("row"), lax.axis_index("col")
    total_rows, depth = fresh.shape
    rows, lcols = left_factor.shape
    dmodel = basis.shape[0]
    width = prod.shape[1]
    ratio = R // C
    H = R // 2
    count = total_rows // m
    hm = m // 2
    keep = xh.shape[0]
    here = place_of(row, R)
    toward = tuple(member_at(lax.rem(here + step, R), R) for step in (1, R - 1))

    def origin_rows(d, j, side=None):
        there = here + R - j if d == 0 else here + j
        first = member_at(lax.rem(there, R), R) * rows
        if side is None:
            return pl.ds(pl.multiple_of(first, 32), rows)
        return pl.ds(pl.multiple_of(first + side * (rows // 2), 32), rows // 2)

    load_v = pltpu.make_async_copy(vectors, bv, load_sem.at[0])
    load_b = pltpu.make_async_copy(basis, lbasis, load_sem.at[1])
    load_f = pltpu.make_async_copy(left_factor, lfac, load_sem.at[2])
    mine = pl.ds(pl.multiple_of(col * lcols, 128), lcols)
    load_p = pltpu.make_async_copy(left_part.at[mine], lparts.at[col], load_sem.at[3])
    load_b.start()
    load_v.start()

    def chunk(k):
        return pltpu.make_async_copy(
            fresh.at[pl.ds(pl.multiple_of(k * m, m), m)], xf.at[lax.rem(k, 2)], x_sem.at[lax.rem(k, 2)])

    chunk(0).start()
    load_f.start()
    load_p.start()
    load_b.wait()
    pieces = [
        pltpu.make_async_copy(piece, lbasis.at[origin_rows(d, H - 1)], load_sem.at[4 + d])
        for d, piece in enumerate((came_forward, came_back))
    ]
    for piece in pieces:
        piece.start()
    greet([{"row": lax.rem(row + j, R)} for j in range(1, R)]
          + [{"col": lax.rem(col + j, C)} for j in range(1, C)])

    def other_col(j):
        return lax.rem(col + j, C)

    def part_copy(j):
        there = other_col(j)
        at = pl.ds(pl.multiple_of(there * lcols, 128), lcols)
        return pltpu.make_async_remote_copy(
            src_ref=left_part.at[at], dst_ref=lparts.at[col],
            send_sem=lp_send.at[j], recv_sem=lp_recv.at[col],
            device_id={"col": there}, device_id_type=MESH)

    def part_in(j):
        source = other_col(j)
        return pltpu.make_async_remote_copy(
            src_ref=left_part.at[mine], dst_ref=lparts.at[source],
            send_sem=lp_send.at[j], recv_sem=lp_recv.at[source],
            device_id={"col": source}, device_id_type=MESH)

    def half_copy(j, source):
        return pltpu.make_async_remote_copy(
            src_ref=lhalf.at[source], dst_ref=lhalf.at[source],
            send_sem=lh_send.at[j], recv_sem=lh_recv.at[source],
            device_id={"col": other_col(j)}, device_id_type=MESH)

    def lsq_copy(j, source):
        return pltpu.make_async_remote_copy(
            src_ref=lsq.at[source], dst_ref=lsq.at[source],
            send_sem=ls_send.at[j], recv_sem=ls_recv.at[source],
            device_id={"row": lax.rem(row + j, R)}, device_id_type=MESH)

    def sq_copy(j, source):
        return pltpu.make_async_remote_copy(
            src_ref=gather_sq.at[source], dst_ref=gather_sq.at[source],
            send_sem=sq_send.at[j], recv_sem=sq_recv.at[source],
            device_id={"col": other_col(j)}, device_id_type=MESH)

    new_out = pltpu.make_async_copy(lnew, left_new_out, out_sem.at[0])
    prod_out = pltpu.make_async_copy(lprod, left_out, out_sem.at[1])

    def left_sum():
        load_p.wait()
        load_f.wait()
        for j in range(1, C):
            part_in(j).wait_recv()
        total = lparts[0]
        for c in range(1, C):
            total = total + lparts[c]
        value = ema_decay * lfac[...] + (1.0 - ema_decay) * total.T
        lnew[...] = value
        lhalf[col] = value.astype(jnp.bfloat16)
        new_out.start()
        for j in range(1, C):
            half_copy(j, col).start()

    def basis_ring(d):
        at = origin_rows(d, H - 1, d)
        return pltpu.make_async_remote_copy(
            src_ref=lbasis.at[at], dst_ref=lbasis.at[at],
            send_sem=lb_send.at[d], recv_sem=lb_recv.at[d],
            device_id={"row": toward[d]}, device_id_type=MESH)

    def left_product():
        for d in range(2):
            basis_ring(d).wait_recv()
        for j in range(1, C):
            half_copy(j, other_col(j)).wait_recv()
        total = None
        for c in range(C):
            term = dot(lhalf[c], lbasis[c * lcols:(c + 1) * lcols], ((1,), (0,)))
            total = term if total is None else total + term
        lprod[...] = total
        lsq[row] = jnp.broadcast_to(jnp.sum(total * total, axis=0, keepdims=True), lsq.shape[1:])
        for j in range(1, R):
            lsq_copy(j, row).start()

    def left_finish():
        for j in range(1, R):
            lsq_copy(j, lax.rem(row + j, R)).wait_recv()
        total = lsq[0]
        for r in range(1, R):
            total = total + lsq[r]
        lprod[...] = lprod[...] * lax.rsqrt(total[0:1] / dmodel + epsilon)
        prod_out.start()

    def message(t, d, h):
        rows = pl.ds(d * hm, hm) if h == 0 else pl.ds(0, m)
        return pltpu.make_async_remote_copy(
            src_ref=sbuf.at[lax.rem(t, 2), d, h, rows],
            dst_ref=rbuf.at[lax.rem(t, 4), d, h, rows],
            send_sem=send_sem.at[lax.rem(t, 2), d, h],
            recv_sem=recv_sem.at[lax.rem(t, 4), d, h],
            device_id={"row": toward[d]}, device_id_type=MESH)

    def block(k, dest, rows):
        source = lax.div(dest, ratio)
        lanes = pl.ds(pl.multiple_of(lax.rem(dest, ratio) * width, 128), width)
        return dot(xh[lax.rem(k, keep), rows], bv[source, :, lanes], ((1,), (0,)))

    def dest_of(d, h):
        away = H - h if d == 0 else R - (H - h)
        return member_at(lax.rem(here + away, R), R)

    def ready(k):
        return jnp.logical_and(k >= 0, k < count)

    for piece in pieces:
        piece.wait()
    for d in range(2):
        basis_ring(d).start()
    for j in range(1, C):
        part_copy(j).start()
    square[...] = jnp.zeros_like(square)
    load_v.wait()
    steps = count + H

    @pl.loop(0, steps)
    def _(t):
        @pl.when(t < count)
        def _():
            chunk(t).wait()

            @pl.when(t + 1 < count)
            def _():
                chunk(t + 1).start()

            xh[lax.rem(t, keep)] = xf[lax.rem(t, 2)].astype(jnp.bfloat16)

        @pl.when(ready(t - H))
        def _():
            k = t - H
            total = block(k, row, slice(0, m))
            for d in range(2):
                message(t - 1, d, H - 1).wait_recv()
                total = total + rbuf[lax.rem(t - 1, 4), d, H - 1].astype(jnp.float32)
            at = pl.ds(pl.multiple_of(k * m, m), m)
            prod[at, :] = total
            pltpu.make_async_copy(prod.at[at], right_out.at[at], out_sem.at[2]).start()
            square[...] += jnp.sum(total * total, axis=0, keepdims=True)

        for h in range(H - 1, -1, -1):
            @pl.when(ready(t - h))
            def _():
                k = t - h
                for d in range(2):
                    @pl.when(k >= 2)
                    def _():
                        message(t - 2, d, h).wait_send()

                    dest = dest_of(d, h)
                    slot = lax.rem(t, 2)
                    some = slice(d * hm, d * hm + hm)
                    rest = slice(hm - d * hm, m - d * hm)
                    if h == 0:
                        sbuf[slot, d, h, some] = block(k, dest, some).astype(jnp.bfloat16)
                    else:
                        fresh_part = block(k, dest, slice(0, m))
                        message(t - 1, d, h - 1).wait_recv()
                        if h == 1:
                            came = rbuf[lax.rem(t - 1, 4), d, 0, some].astype(jnp.float32)
                            sbuf[slot, d, h, some] = (fresh_part[some] + came).astype(jnp.bfloat16)
                            sbuf[slot, d, h, rest] = fresh_part[rest].astype(jnp.bfloat16)
                        else:
                            came = rbuf[lax.rem(t - 1, 4), d, h - 1].astype(jnp.float32)
                            sbuf[slot, d, h] = (fresh_part + came).astype(jnp.bfloat16)
                    message(t, d, h).start()

        work = [(6, left_sum), (8, left_product), (10, left_finish)]
        for at, run in work:
            pl.when(t == min(at, steps - 1))(run)

    gather_sq[col] = jnp.broadcast_to(square[...], gather_sq.shape[1:])
    for j in range(1, C):
        sq_copy(j, col).start()
    for d in range(2):
        for h in range(H):
            for k in (count - 2, count - 1):
                message(k + h, d, h).wait_send()
    for j in range(1, C):
        part_copy(j).wait_send()
        half_copy(j, col).wait_send()
    for j in range(1, R):
        lsq_copy(j, row).wait_send()
    for d in range(2):
        basis_ring(d).wait_send()
    new_out.wait()
    prod_out.wait()
    for j in range(1, C):
        sq_copy(j, other_col(j)).wait_recv()
    total = gather_sq[0]
    for c in range(1, C):
        total = total + gather_sq[c]
    sum_sq[...] = total
    put_sq = pltpu.make_async_copy(sum_sq, square_out, out_sem.at[3])
    put_sq.start()
    for j in range(1, C):
        sq_copy(j, col).wait_send()
    put_sq.wait()
    pltpu.make_async_copy(prod, right_out, out_sem.at[2]).wait()


def product_stage(R, C, dhidden, fresh, vectors, left_part, basis, came, left_factor):
    total_rows, depth = fresh.shape
    m = CHUNK
    H = R // 2
    width = vectors.shape[0] * vectors.shape[2] // R
    rows, lcols = left_factor.shape
    any_space = pl.BlockSpec(memory_space=pl.ANY)
    dma = pltpu.SemaphoreType.DMA
    f32, bf16 = jnp.float32, jnp.bfloat16
    return pl.pallas_call(
        functools.partial(product_kernel, R, C, m, dhidden),
        out_shape=(
            jax.ShapeDtypeStruct((total_rows, width), f32),
            jax.ShapeDtypeStruct((8, width), f32),
            jax.ShapeDtypeStruct((rows, lcols), f32),
            jax.ShapeDtypeStruct((rows, lcols), f32),
        ),
        in_specs=[any_space] * 7,
        out_specs=(any_space,) * 4,
        scratch_shapes=[
            pltpu.VMEM(vectors.shape, bf16),
            pltpu.VMEM((2, m, depth), f32),
            pltpu.VMEM((H + 1, m, depth), bf16),
            pltpu.VMEM((4, 2, H, m, width), bf16),
            pltpu.VMEM((2, 2, H, m, width), bf16),
            pltpu.VMEM((total_rows, width), f32),
            pltpu.VMEM((1, width), f32),
            pltpu.VMEM((C, 8, width), f32),
            pltpu.VMEM((8, width), f32),
            pltpu.VMEM((C, lcols, rows), f32),
            pltpu.VMEM((C, rows, lcols), bf16),
            pltpu.VMEM(basis.shape, bf16),
            pltpu.VMEM((rows, lcols), f32),
            pltpu.VMEM((rows, lcols), f32),
            pltpu.VMEM((rows, lcols), f32),
            pltpu.VMEM((R, 8, lcols), f32),
            dma((6,)), dma((2,)), dma((2, 2, H)), dma((4, 2, H)), dma((C,)), dma((C,)),
            dma((C,)), dma((C,)), dma((C,)), dma((C,)), dma((R,)), dma((R,)), dma((2,)), dma((2,)), dma((4,)),
        ],
        compiler_params=pltpu.CompilerParams(
            collective_id=1, has_side_effects=True, vmem_limit_bytes=62 * 1024 * 1024),
        name="product_reduce",
    )(fresh, vectors, left_part, basis, *came, left_factor)


def finish_kernel(dhidden, prod, square, left_new, left_prod, right_out, left_new_out, left_out):
    right_out[...] = prod[...] * lax.rsqrt(square[0:1] / dhidden + epsilon)
    left_new_out[...] = left_new[...]
    left_out[...] = left_prod[...]


def finish_stage(dhidden, prod, square, left_new, left_prod):
    steps = 4
    blocks = [
        pl.BlockSpec((a.shape[0] // steps, a.shape[1]), lambda i: (i, 0))
        for a in (prod, left_new, left_prod)
    ]
    return pl.pallas_call(
        functools.partial(finish_kernel, dhidden),
        grid=(steps,),
        out_shape=tuple(jax.ShapeDtypeStruct(a.shape, a.dtype) for a in (prod, left_new, left_prod)),
        in_specs=[blocks[0], pl.BlockSpec(square.shape, lambda i: (0, 0)), blocks[1], blocks[2]],
        out_specs=tuple(blocks),
        name="finish",
    )(prod, square, left_new, left_prod)


def make_body(R, C, dhidden):
    members = [2 * p if p < R // 2 else 2 * (R - 1 - p) + 1 for p in range(R)]
    forward = [(members[p], members[(p + 1) % R]) for p in range(R)]
    backward = [(b, a) for a, b in forward]

    def on_device(gradient, left_factor, right_factor, left_basis, right_basis):
        row = lax.axis_index("row")
        here = place_of(row, R)
        partial, gram_part, left_basis_cols, vectors, last, match, _ = gather_stage(
            R, C, gradient, left_basis, right_basis, right_factor)
        rows = left_basis.shape[0]
        held = R // 2 - 2
        came = []
        for perm, away in ((forward, R - held), (backward, held)):
            start = member_at(lax.rem(here + away, R), R) * rows
            piece = lax.dynamic_slice_in_dim(left_basis_cols, start, rows, 0)
            came.append(lax.ppermute(piece, "row", perm))
        last, match = (a.reshape(-1, a.shape[-1]) for a in (last, match))
        right_new = partial + (1.0 - ema_decay) * dot(last, match, ((0,), (0,)))
        right_prod, square, left_new, left_out = product_stage(
            R, C, dhidden, right_new, vectors, gram_part, left_basis_cols, came, left_factor)
        right_out, left_new, left_out = finish_stage(dhidden, right_prod, square, left_new, left_out)
        return (left_new, right_new, left_out, right_out)

    return on_device


def solution(mesh):
    in_specs = (P("row", "col"), P("row", "col"), P("col", "row"), P("row", "col"), P("row", "col"))
    out_specs = (P("row", "col"), P("col", "row"), P("row", "col"), P("col", "row"))

    def step(gradient, left_factor, right_factor, left_basis, right_basis):
        body = make_body(mesh.shape["row"], mesh.shape["col"], gradient.shape[1])
        return jax.shard_map(
            body, mesh=mesh, in_specs=in_specs, out_specs=out_specs, check_vma=False
        )(gradient, left_factor, right_factor, left_basis, right_basis)

    return step
```

```python
import functools

import jax
import jax.numpy as jnp
from jax import lax
from jax.experimental import pallas as pl
from jax.experimental.pallas import tpu as pltpu
from jax.sharding import PartitionSpec as P

ema_decay = 0.95
epsilon = 1e-06
MESH = pl.DeviceIdType.MESH
SLOTS = 4
SPLIT = 2
CHUNK = 256


def dot(a, b, dims):
    return lax.dot_general(a, b, (dims, ((), ())), preferred_element_type=jnp.float32)


def place_of(row, row_count):
    half = lax.div(row, 2)
    return jnp.where(lax.rem(row, 2) == 0, half, row_count - 1 - half)


def member_at(place, row_count):
    return jnp.where(place < row_count // 2, 2 * place, 2 * (row_count - 1 - place) + 1)


def greet(peers):
    barrier = pltpu.get_barrier_semaphore()
    for peer in peers:
        pl.semaphore_signal(barrier, inc=1, device_id=peer, device_id_type=MESH)
    pl.semaphore_wait(barrier, len(peers))


def gather_kernel(
    R, C, tile,
    grad, lb, rb, rf,
    partial_out, left_out, lb_out, rb_out, last_out, last_match, match,
    acc, slab, own, rhs, left,
    load_sem, rf_sem, ring_send, ring_recv, match_send, match_recv, rhs_sem,
    lb_send, lb_recv, rb_send, rb_recv, keep_sem, out_sem,
):
    row, col = lax.axis_index("row"), lax.axis_index("col")
    rows, cols = grad.shape
    half = rows // 2
    ratio = R // C
    part = cols // ratio
    here = place_of(row, R)
    nxt = member_at(lax.rem(here + 1, R), R)
    prv = member_at(lax.rem(here + R - 1, R), R)
    toward = (nxt, prv)
    owner = lax.div(row, ratio)
    quarter = half // SPLIT
    chosen = pl.ds(pl.multiple_of(lax.rem(row, ratio) * part, 128), part)
    last = R - 1
    offset = lax.rem(col + C - owner, C)
    is_owner = offset == 0
    is_relay = jnp.logical_and(offset != 0, lax.rem(offset, 2) == 0)
    partner = col + 1 - 2 * lax.rem(col, 2)

    def origin(direction, t):
        there = here + R - t if direction == 0 else here + t
        return member_at(lax.rem(there, R), R)

    loads = [pltpu.make_async_copy(grad, own, load_sem.at[2, 0])]
    for s in range(SPLIT):
        for d in range(2):
            loads.append(pltpu.make_async_copy(
                grad.at[pl.ds(d * half + s * quarter, quarter)], slab.at[0, d, s], load_sem.at[d, s]))
    for load in reversed(loads):
        load.start()
    load_rf = pltpu.make_async_copy(rf, acc, rf_sem)
    load_rf.start()
    keep_lb = pltpu.make_async_copy(
        lb, lb_out.at[pl.ds(pl.multiple_of(row * rows, 32), rows)], keep_sem.at[0])
    keep_rb = pltpu.make_async_copy(rb, rb_out.at[col], keep_sem.at[1])

    greet([{"row": nxt}, {"row": prv}] + [{"col": lax.rem(col + j, C)} for j in range(1, C)])

    def ring(t, d, s):
        return pltpu.make_async_remote_copy(
            src_ref=slab.at[t % SLOTS, d, s],
            dst_ref=slab.at[(t + 1) % SLOTS, d, s],
            send_sem=ring_send.at[t % 2, d, s],
            recv_sem=ring_recv.at[(t + 1) % SLOTS, d, s],
            device_id={"row": toward[d]}, device_id_type=MESH)

    def landed(t, d, s):
        return last_match.at[d, s] if t == last else match.at[t, d, s]

    def match_copy(t, d, s, j, source):
        target = partner if j == 0 else lax.rem(col + 2 * j, C)
        return pltpu.make_async_remote_copy(
            src_ref=source, dst_ref=landed(t, d, s),
            send_sem=match_send.at[t % 2, d, s, j], recv_sem=match_recv.at[t, d, s],
            device_id={"col": target}, device_id_type=MESH)

    def offers(t, s):
        return [match_copy(t, d, s, j, slab.at[t % SLOTS, d, s, :, chosen])
                for d in range(2) for j in list(range(1, C // 2)) + [0]]

    def relays(t, s):
        return [match_copy(t, d, s, 0, landed(t, d, s)) for d in range(2)]

    def offer(t, s):
        @pl.when(is_owner)
        def _():
            for copy in offers(t, s):
                copy.start()

    def settle(t):
        for s in range(SPLIT):
            @pl.when(is_owner)
            def _():
                for copy in offers(t, s):
                    copy.wait_send()

            @pl.when(is_relay)
            def _():
                for copy in relays(t, s):
                    copy.wait_send()

    def relay(t, s):
        @pl.when(is_relay)
        def _():
            for copy in relays(t, s):
                copy.wait_recv()
                copy.start()

    def arrive(t):
        @pl.when(jnp.logical_not(jnp.logical_or(is_owner, is_relay)))
        def _():
            for s in range(SPLIT):
                for copy in relays(t, s):
                    copy.wait_recv()

    def bring(t):
        arrive(t)

        @pl.when(is_owner)
        def _():
            for d in range(2):
                for s in range(SPLIT):
                    rhs[t % 2, d, s] = slab[t % SLOTS, d, s, :, chosen]

        @pl.when(jnp.logical_not(is_owner))
        def _():
            copy = pltpu.make_async_copy(match.at[t], rhs.at[t % 2], rhs_sem.at[0])
            copy.start()
            copy.wait()

    def write(row0):
        return pltpu.make_async_copy(
            acc.at[pl.ds(row0, tile)], partial_out.at[pl.ds(row0, tile)], out_sem)

    def gram(t, s):
        @pl.loop(0, part // tile)
        def _(j):
            first = pl.multiple_of(j * tile, tile)
            row0 = pl.multiple_of(s * part + first, tile)
            block = slab[t % SLOTS, :, :, :, pl.ds(row0, tile)].reshape(rows, tile).T
            for n in range(part // tile):
                lanes = slice(n * tile, (n + 1) * tile)
                other = rhs[t % 2, :, :, :, lanes].reshape(rows, tile)
                acc[pl.ds(row0, tile), lanes] += (1.0 - ema_decay) * dot(block, other, ((1,), (0,)))
            if t == last - 1:
                write(row0).start()

    def gram_left(t):
        for d in range(2):
            total = dot(slab[t % SLOTS, d].reshape(half, cols), own[...], ((1,), (1,)))
            row0 = pl.multiple_of(origin(d, t) * rows + d * half, 32)
            left[pl.ds(row0, half), :] = total

    def basis_ring(j, d):
        at = pl.ds(pl.multiple_of(origin(d, j) * rows, 32), rows)
        return pltpu.make_async_remote_copy(
            src_ref=lb if j == 0 else lb_out.at[at], dst_ref=lb_out.at[at],
            send_sem=lb_send.at[j % 2, d], recv_sem=lb_recv.at[j, d],
            device_id={"row": toward[d]}, device_id_type=MESH)

    def basis_hop(j):
        for d in range(2):
            if j > 0:
                basis_ring(j - 1, d).wait_recv()
        for d in range(2):
            if j < hops:
                if j > 1:
                    basis_ring(j - 2, d).wait_send()
                basis_ring(j, d).start()

    def vectors(j):
        target = partner if j == 0 else lax.rem(col + 2 * j, C)
        return pltpu.make_async_remote_copy(
            src_ref=rb, dst_ref=rb_out.at[col], send_sem=rb_send.at[0, j], recv_sem=rb_recv.at[col],
            device_id={"col": target}, device_id_type=MESH)

    def vectors_on(j):
        source = lax.rem(col + 2 * j, C)
        return pltpu.make_async_remote_copy(
            src_ref=rb_out.at[source], dst_ref=rb_out.at[source],
            send_sem=rb_send.at[1, j], recv_sem=rb_recv.at[source],
            device_id={"col": partner}, device_id_type=MESH)

    def vectors_in(source):
        return pltpu.make_async_remote_copy(
            src_ref=rb, dst_ref=rb_out.at[source], send_sem=rb_send.at[0, 0], recv_sem=rb_recv.at[source],
            device_id={"col": partner}, device_id_type=MESH)

    for load in reversed(loads):
        load.wait()
    for s in range(SPLIT):
        for d in range(2):
            ring(0, d, s).start()
    for s in range(SPLIT):
        offer(0, s)
    keep_lb.start()
    keep_rb.start()
    for j in range(C // 2):
        vectors(j).start()
    load_rf.wait()

    @pl.loop(0, cols // tile)
    def _(j):
        at = pl.ds(pl.multiple_of(j * tile, tile), tile)
        acc[at, :] = acc[at, :] * ema_decay

    relay_due = [(0, s) for s in range(SPLIT)]
    hops = R // 2 - 2
    begin = R - 1 - hops
    for t in range(1, R):
        for s in range(SPLIT):
            for d in range(2):
                ring(t - 1, d, s).wait_recv()
            if t < last:
                for d in range(2):
                    ring(t, d, s).start()
            offer(t, s)
            if s == SPLIT - 1 and begin <= t < last:
                basis_hop(t - begin)
            for due in relay_due:
                relay(*due)
            relay_due = [(t, s)]
            if s == 0:
                bring(t - 1)
            if s < SPLIT - 1:
                gram(t - 1, s)
            else:
                for rest in range(s, ratio):
                    gram(t - 1, rest)
                gram_left(t - 1)
                settle(t - 1)
            for d in range(2):
                ring(t - 1, d, s).wait_send()
        if t == R // 2 - 1:
            for j in range(1, C // 2):
                vectors_in(lax.rem(col + 2 * j, C)).wait_recv()
                vectors_on(j).start()
    put_last = pltpu.make_async_copy(slab.at[last % SLOTS], last_out, keep_sem.at[3])
    put_last.start()
    own_match = pltpu.make_async_copy(slab.at[last % SLOTS, :, :, :, chosen], last_match, rhs_sem.at[1])

    @pl.when(is_owner)
    def _():
        own_match.start()

    gram_left(last)
    put_left = pltpu.make_async_copy(left, left_out, keep_sem.at[2])
    put_left.start()
    for due in relay_due:
        relay(*due)
    arrive(last)
    settle(last)
    basis_hop(hops)
    for d in range(2):
        for j in range(max(hops - 2, 0), hops):
            basis_ring(j, d).wait_send()

    @pl.when(is_owner)
    def _():
        own_match.wait()

    put_last.wait()
    keep_lb.wait()
    keep_rb.wait()
    vectors_in(partner).wait_recv()
    for j in range(1, C // 2):
        vectors_in(lax.rem(partner + 2 * j, C)).wait_recv()
        vectors_on(j).wait_send()
    for j in range(C // 2):
        vectors(j).wait_send()
    put_left.wait()
    pltpu.make_async_copy(acc, partial_out, out_sem).wait()


def gather_stage(R, C, gradient, left_basis, right_basis, right_factor):
    rows, cols = gradient.shape
    half, ratio = rows // 2, R // C
    part, quarter = cols // ratio, half // SPLIT
    tile = 256 if part % 256 == 0 else 128
    dmodel = rows * R
    any_space = pl.BlockSpec(memory_space=pl.ANY)
    dma = pltpu.SemaphoreType.DMA
    return pl.pallas_call(
        functools.partial(gather_kernel, R, C, tile),
        out_shape=(
            jax.ShapeDtypeStruct(right_factor.shape, jnp.float32),
            jax.ShapeDtypeStruct((dmodel, rows), jnp.float32),
            jax.ShapeDtypeStruct((dmodel, left_basis.shape[1]), jnp.bfloat16),
            jax.ShapeDtypeStruct((C,) + right_basis.shape, jnp.bfloat16),
            jax.ShapeDtypeStruct((2, SPLIT, quarter, cols), jnp.bfloat16),
            jax.ShapeDtypeStruct((2, SPLIT, quarter, part), jnp.bfloat16),
            jax.ShapeDtypeStruct((R - 1, 2, SPLIT, quarter, part), jnp.bfloat16),
        ),
        in_specs=[any_space] * 4,
        out_specs=(any_space,) * 7,
        scratch_shapes=[
            pltpu.VMEM(right_factor.shape, jnp.float32),
            pltpu.VMEM((SLOTS, 2, SPLIT, quarter, cols), jnp.bfloat16),
            pltpu.VMEM((rows, cols), jnp.bfloat16),
            pltpu.VMEM((2, 2, SPLIT, quarter, part), jnp.bfloat16),
            pltpu.VMEM((dmodel, rows), jnp.float32),
            dma((3, SPLIT)), dma, dma((2, 2, SPLIT)), dma((SLOTS, 2, SPLIT)),
            dma((2, 2, SPLIT, C // 2)), dma((R, 2, SPLIT)), dma((2,)),
            dma((2, 2)), dma((R - 1, 2)), dma((2, C // 2)), dma((C,)), dma((4,)), dma,
        ],
        compiler_params=pltpu.CompilerParams(
            collective_id=0, has_side_effects=True, vmem_limit_bytes=62 * 1024 * 1024),
        name="gather_gram",
    )(gradient, left_basis, right_basis, right_factor)


def product_kernel(
    R, C, m, dhidden,
    fresh, vectors, left_part, basis, came_forward, came_back, left_factor,
    right_out, square_out, left_new_out, left_out,
    bv, xf, xh, rbuf, sbuf, prod, square, gather_sq, sum_sq,
    lparts, lhalf, lbasis, lfac, lnew, lprod, lsq,
    load_sem, x_sem, send_sem, recv_sem, sq_send, sq_recv,
    lp_send, lp_recv, lh_send, lh_recv, ls_send, ls_recv, lb_send, lb_recv, out_sem,
):
    row, col = lax.axis_index("row"), lax.axis_index("col")
    total_rows, depth = fresh.shape
    rows, lcols = left_factor.shape
    dmodel = basis.shape[0]
    width = prod.shape[1]
    ratio = R // C
    H = R // 2
    count = total_rows // m
    hm = m // 2
    keep = xh.shape[0]
    here = place_of(row, R)
    toward = tuple(member_at(lax.rem(here + step, R), R) for step in (1, R - 1))

    def origin_rows(d, j, side=None):
        there = here + R - j if d == 0 else here + j
        first = member_at(lax.rem(there, R), R) * rows
        if side is None:
            return pl.ds(pl.multiple_of(first, 32), rows)
        return pl.ds(pl.multiple_of(first + side * (rows // 2), 32), rows // 2)

    load_v = pltpu.make_async_copy(vectors, bv, load_sem.at[0])
    load_b = pltpu.make_async_copy(basis, lbasis, load_sem.at[1])
    load_f = pltpu.make_async_copy(left_factor, lfac, load_sem.at[2])
    mine = pl.ds(pl.multiple_of(col * lcols, 128), lcols)
    load_p = pltpu.make_async_copy(left_part.at[mine], lparts.at[col], load_sem.at[3])
    load_b.start()
    load_v.start()

    def chunk(k):
        return pltpu.make_async_copy(
            fresh.at[pl.ds(pl.multiple_of(k * m, m), m)], xf.at[lax.rem(k, 2)], x_sem.at[lax.rem(k, 2)])

    chunk(0).start()
    load_f.start()
    load_p.start()
    load_b.wait()
    pieces = [
        pltpu.make_async_copy(piece, lbasis.at[origin_rows(d, H - 1)], load_sem.at[4 + d])
        for d, piece in enumerate((came_forward, came_back))
    ]
    for piece in pieces:
        piece.start()
    greet([{"row": lax.rem(row + j, R)} for j in range(1, R)]
          + [{"col": lax.rem(col + j, C)} for j in range(1, C)])

    def other_col(j):
        return lax.rem(col + j, C)

    def part_copy(j):
        there = other_col(j)
        at = pl.ds(pl.multiple_of(there * lcols, 128), lcols)
        return pltpu.make_async_remote_copy(
            src_ref=left_part.at[at], dst_ref=lparts.at[col],
            send_sem=lp_send.at[j], recv_sem=lp_recv.at[col],
            device_id={"col": there}, device_id_type=MESH)

    def part_in(j):
        source = other_col(j)
        return pltpu.make_async_remote_copy(
            src_ref=left_part.at[mine], dst_ref=lparts.at[source],
            send_sem=lp_send.at[j], recv_sem=lp_recv.at[source],
            device_id={"col": source}, device_id_type=MESH)

    def half_copy(j, source):
        return pltpu.make_async_remote_copy(
            src_ref=lhalf.at[source], dst_ref=lhalf.at[source],
            send_sem=lh_send.at[j], recv_sem=lh_recv.at[source],
            device_id={"col": other_col(j)}, device_id_type=MESH)

    def lsq_copy(j, source):
        return pltpu.make_async_remote_copy(
            src_ref=lsq.at[source], dst_ref=lsq.at[source],
            send_sem=ls_send.at[j], recv_sem=ls_recv.at[source],
            device_id={"row": lax.rem(row + j, R)}, device_id_type=MESH)

    def sq_copy(j, source):
        return pltpu.make_async_remote_copy(
            src_ref=gather_sq.at[source], dst_ref=gather_sq.at[source],
            send_sem=sq_send.at[j], recv_sem=sq_recv.at[source],
            device_id={"col": other_col(j)}, device_id_type=MESH)

    new_out = pltpu.make_async_copy(lnew, left_new_out, out_sem.at[0])
    prod_out = pltpu.make_async_copy(lprod, left_out, out_sem.at[1])

    def left_sum():
        load_p.wait()
        load_f.wait()
        for j in range(1, C):
            part_in(j).wait_recv()
        total = lparts[0]
        for c in range(1, C):
            total = total + lparts[c]
        value = ema_decay * lfac[...] + (1.0 - ema_decay) * total.T
        lnew[...] = value
        lhalf[col] = value.astype(jnp.bfloat16)
        new_out.start()
        for j in range(1, C):
            half_copy(j, col).start()

    def basis_ring(d):
        at = origin_rows(d, H - 1, d)
        return pltpu.make_async_remote_copy(
            src_ref=lbasis.at[at], dst_ref=lbasis.at[at],
            send_sem=lb_send.at[d], recv_sem=lb_recv.at[d],
            device_id={"row": toward[d]}, device_id_type=MESH)

    def left_product():
        for d in range(2):
            basis_ring(d).wait_recv()
        for j in range(1, C):
            half_copy(j, other_col(j)).wait_recv()
        total = None
        for c in range(C):
            term = dot(lhalf[c], lbasis[c * lcols:(c + 1) * lcols], ((1,), (0,)))
            total = term if total is None else total + term
        lprod[...] = total
        lsq[row] = jnp.broadcast_to(jnp.sum(total * total, axis=0, keepdims=True), lsq.shape[1:])
        for j in range(1, R):
            lsq_copy(j, row).start()

    def left_finish():
        for j in range(1, R):
            lsq_copy(j, lax.rem(row + j, R)).wait_recv()
        total = lsq[0]
        for r in range(1, R):
            total = total + lsq[r]
        lprod[...] = lprod[...] * lax.rsqrt(total[0:1] / dmodel + epsilon)
        prod_out.start()

    def message(t, d, h):
        rows = pl.ds(d * hm, hm) if h == 0 else pl.ds(0, m)
        return pltpu.make_async_remote_copy(
            src_ref=sbuf.at[lax.rem(t, 2), d, h, rows],
            dst_ref=rbuf.at[lax.rem(t, 4), d, h, rows],
            send_sem=send_sem.at[lax.rem(t, 2), d, h],
            recv_sem=recv_sem.at[lax.rem(t, 4), d, h],
            device_id={"row": toward[d]}, device_id_type=MESH)

    def block(k, dest, rows):
        source = lax.div(dest, ratio)
        lanes = pl.ds(pl.multiple_of(lax.rem(dest, ratio) * width, 128), width)
        return dot(xh[lax.rem(k, keep), rows], bv[source, :, lanes], ((1,), (0,)))

    def dest_of(d, h):
        away = H - h if d == 0 else R - (H - h)
        return member_at(lax.rem(here + away, R), R)

    def ready(k):
        return jnp.logical_and(k >= 0, k < count)

    for piece in pieces:
        piece.wait()
    for d in range(2):
        basis_ring(d).start()
    for j in range(1, C):
        part_copy(j).start()
    square[...] = jnp.zeros_like(square)
    load_v.wait()
    steps = count + H

    @pl.loop(0, steps)
    def _(t):
        @pl.when(t < count)
        def _():
            chunk(t).wait()

            @pl.when(t + 1 < count)
            def _():
                chunk(t + 1).start()

            xh[lax.rem(t, keep)] = xf[lax.rem(t, 2)].astype(jnp.bfloat16)

        @pl.when(ready(t - H))
        def _():
            k = t - H
            total = block(k, row, slice(0, m))
            for d in range(2):
                message(t - 1, d, H - 1).wait_recv()
                total = total + rbuf[lax.rem(t - 1, 4), d, H - 1].astype(jnp.float32)
            at = pl.ds(pl.multiple_of(k * m, m), m)
            prod[at, :] = total
            pltpu.make_async_copy(prod.at[at], right_out.at[at], out_sem.at[2]).start()
            square[...] += jnp.sum(total * total, axis=0, keepdims=True)

        for h in range(H - 1, -1, -1):
            @pl.when(ready(t - h))
            def _():
                k = t - h
                for d in range(2):
                    @pl.when(k >= 2)
                    def _():
                        message(t - 2, d, h).wait_send()

                    dest = dest_of(d, h)
                    slot = lax.rem(t, 2)
                    some = slice(d * hm, d * hm + hm)
                    rest = slice(hm - d * hm, m - d * hm)
                    if h == 0:
                        sbuf[slot, d, h, some] = block(k, dest, some).astype(jnp.bfloat16)
                    else:
                        fresh_part = block(k, dest, slice(0, m))
                        message(t - 1, d, h - 1).wait_recv()
                        if h == 1:
                            came = rbuf[lax.rem(t - 1, 4), d, 0, some].astype(jnp.float32)
                            sbuf[slot, d, h, some] = (fresh_part[some] + came).astype(jnp.bfloat16)
                            sbuf[slot, d, h, rest] = fresh_part[rest].astype(jnp.bfloat16)
                        else:
                            came = rbuf[lax.rem(t - 1, 4), d, h - 1].astype(jnp.float32)
                            sbuf[slot, d, h] = (fresh_part + came).astype(jnp.bfloat16)
                    message(t, d, h).start()

        work = [(6, left_sum), (8, left_product), (10, left_finish)]
        for at, run in work:
            pl.when(t == min(at, steps - 1))(run)

    gather_sq[col] = jnp.broadcast_to(square[...], gather_sq.shape[1:])
    for j in range(1, C):
        sq_copy(j, col).start()
    for d in range(2):
        for h in range(H):
            for k in (count - 2, count - 1):
                message(k + h, d, h).wait_send()
    for j in range(1, C):
        part_copy(j).wait_send()
        half_copy(j, col).wait_send()
    for j in range(1, R):
        lsq_copy(j, row).wait_send()
    for d in range(2):
        basis_ring(d).wait_send()
    new_out.wait()
    prod_out.wait()
    for j in range(1, C):
        sq_copy(j, other_col(j)).wait_recv()
    total = gather_sq[0]
    for c in range(1, C):
        total = total + gather_sq[c]
    sum_sq[...] = total
    put_sq = pltpu.make_async_copy(sum_sq, square_out, out_sem.at[3])
    put_sq.start()
    for j in range(1, C):
        sq_copy(j, col).wait_send()
    put_sq.wait()
    pltpu.make_async_copy(prod, right_out, out_sem.at[2]).wait()


def product_stage(R, C, dhidden, fresh, vectors, left_part, basis, came, left_factor):
    total_rows, depth = fresh.shape
    m = CHUNK
    H = R // 2
    width = vectors.shape[0] * vectors.shape[2] // R
    rows, lcols = left_factor.shape
    any_space = pl.BlockSpec(memory_space=pl.ANY)
    dma = pltpu.SemaphoreType.DMA
    f32, bf16 = jnp.float32, jnp.bfloat16
    return pl.pallas_call(
        functools.partial(product_kernel, R, C, m, dhidden),
        out_shape=(
            jax.ShapeDtypeStruct((total_rows, width), f32),
            jax.ShapeDtypeStruct((8, width), f32),
            jax.ShapeDtypeStruct((rows, lcols), f32),
            jax.ShapeDtypeStruct((rows, lcols), f32),
        ),
        in_specs=[any_space] * 7,
        out_specs=(any_space,) * 4,
        scratch_shapes=[
            pltpu.VMEM(vectors.shape, bf16),
            pltpu.VMEM((2, m, depth), f32),
            pltpu.VMEM((H + 1, m, depth), bf16),
            pltpu.VMEM((4, 2, H, m, width), bf16),
            pltpu.VMEM((2, 2, H, m, width), bf16),
            pltpu.VMEM((total_rows, width), f32),
            pltpu.VMEM((1, width), f32),
            pltpu.VMEM((C, 8, width), f32),
            pltpu.VMEM((8, width), f32),
            pltpu.VMEM((C, lcols, rows), f32),
            pltpu.VMEM((C, rows, lcols), bf16),
            pltpu.VMEM(basis.shape, bf16),
            pltpu.VMEM((rows, lcols), f32),
            pltpu.VMEM((rows, lcols), f32),
            pltpu.VMEM((rows, lcols), f32),
            pltpu.VMEM((R, 8, lcols), f32),
            dma((6,)), dma((2,)), dma((2, 2, H)), dma((4, 2, H)), dma((C,)), dma((C,)),
            dma((C,)), dma((C,)), dma((C,)), dma((C,)), dma((R,)), dma((R,)), dma((2,)), dma((2,)), dma((4,)),
        ],
        compiler_params=pltpu.CompilerParams(
            collective_id=1, has_side_effects=True, vmem_limit_bytes=62 * 1024 * 1024),
        name="product_reduce",
    )(fresh, vectors, left_part, basis, *came, left_factor)


def finish_kernel(dhidden, prod, square, left_new, left_prod, right_out, left_new_out, left_out):
    right_out[...] = prod[...] * lax.rsqrt(square[0:1] / dhidden + epsilon)
    left_new_out[...] = left_new[...]
    left_out[...] = left_prod[...]


def finish_stage(dhidden, prod, square, left_new, left_prod):
    steps = 4
    blocks = [
        pl.BlockSpec((a.shape[0] // steps, a.shape[1]), lambda i: (i, 0))
        for a in (prod, left_new, left_prod)
    ]
    return pl.pallas_call(
        functools.partial(finish_kernel, dhidden),
        grid=(steps,),
        out_shape=tuple(jax.ShapeDtypeStruct(a.shape, a.dtype) for a in (prod, left_new, left_prod)),
        in_specs=[blocks[0], pl.BlockSpec(square.shape, lambda i: (0, 0)), blocks[1], blocks[2]],
        out_specs=tuple(blocks),
        name="finish",
    )(prod, square, left_new, left_prod)


def make_body(R, C, dhidden):
    members = [2 * p if p < R // 2 else 2 * (R - 1 - p) + 1 for p in range(R)]
    forward = [(members[p], members[(p + 1) % R]) for p in range(R)]
    backward = [(b, a) for a, b in forward]

    def on_device(gradient, left_factor, right_factor, left_basis, right_basis):
        row = lax.axis_index("row")
        here = place_of(row, R)
        partial, gram_part, left_basis_cols, vectors, last, match, _ = gather_stage(
            R, C, gradient, left_basis, right_basis, right_factor)
        rows = left_basis.shape[0]
        held = R // 2 - 2
        came = []
        for perm, away in ((forward, R - held), (backward, held)):
            start = member_at(lax.rem(here + away, R), R) * rows
            piece = lax.dynamic_slice_in_dim(left_basis_cols, start, rows, 0)
            came.append(lax.ppermute(piece, "row", perm))
        last, match = (a.reshape(-1, a.shape[-1]) for a in (last, match))
        right_new = partial + (1.0 - ema_decay) * dot(last, match, ((0,), (0,)))
        right_prod, square, left_new, left_out = product_stage(
            R, C, dhidden, right_new, vectors, gram_part, left_basis_cols, came, left_factor)
        right_out, left_new, left_out = finish_stage(dhidden, right_prod, square, left_new, left_out)
        return (left_new, right_new, left_out, right_out)

    return on_device


def solution(mesh):
    in_specs = (P("row", "col"), P("row", "col"), P("col", "row"), P("row", "col"), P("row", "col"))
    out_specs = (P("row", "col"), P("col", "row"), P("row", "col"), P("col", "row"))

    def step(gradient, left_factor, right_factor, left_basis, right_basis):
        body = make_body(mesh.shape["row"], mesh.shape["col"], gradient.shape[1])
        return jax.shard_map(
            body, mesh=mesh, in_specs=in_specs, out_specs=out_specs, check_vma=False
        )(gradient, left_factor, right_factor, left_basis, right_basis)

    return step
```
